256 devices in a mesh: io: 4 (over y_hi, core), comp: 64 (over y_lo, x, z).
Axes of the slice: x: 4, y: 4 (y_hi: 2, y_lo: 2; y = y_hi * 2 + y_lo), z: 8, core: 2. Of those that a mesh axis runs over, the one named last changes fastest.
Arguments:
- fields: float32 [786432, 256], P(('io', 'comp')), may hold values from -6 to 6
- file_offset: int32 [6144, 128], P(('io', 'comp')), may hold values from 0 to 786431, as said below
- level_remap: float32 [4, 64, 64], replicated, may hold values from -0.75 to 0.75
Outputs:
- history: float32 [786432, 256], P(('io', 'comp'))
The draws below stay inside these ranges and needn't reach their ends.
Inputs may be any that keep to these rules, and one draw needn't show every extreme that they name: file_offset is a permutation of the 786432 file positions. The owner of a position p is the device of flat index p // 3072 (io index times the comp size plus comp index). A device's columns have as owners only itself, devices of its io index and devices of its comp index. To each other device of its io index it sends exactly 8 columns, except the two of comp index one above and one below (cyclically), which get 8 plus between 96 and 192; likewise along io with the devices of its comp index. Two neighbours exchange equally many columns each way, and the count 8 + 192 is reached in every draw. Which columns and positions is drawn.
All inputs are finite; a program needn't handle non-finite values.
Results may differ from the reference program's by a relative error of at most 0.00005.
Values sent between devices are 32-bit elements; how exact they have to be, the bound alone decides.
No kernel may reach another device: no remote copies, remote signals or barrier semaphores. Data moves between devices by JAX's collectives and lax.ppermute only.
A program may use at most 64 MiB of HBM per device.

```python
import jax
import jax.numpy as jnp
from jax import lax

FIELDS = 4
LEV = 64
COLS_DEV = 3072
SPREAD = 8
MOST = 192
COLS = 786432
N_IO = 4
N_COMP = 64


def draw_file_offset(key, part):
    group_count = N_IO
    task_count = N_COMP
    device_count = group_count * task_count
    keys = jax.random.split(jax.random.fold_in(key, 11), 7)
    lowest = MOST // 2
    comp_pairs = jax.random.randint(keys[0], (group_count, task_count), lowest, MOST + 1)
    comp_pairs = comp_pairs.at[jnp.arange(group_count), jax.random.randint(keys[1], (group_count,), 0, task_count)].set(MOST)
    io_pairs = jax.random.randint(keys[2], (group_count, task_count), lowest, MOST + 1)
    io_pairs = io_pairs.at[jax.random.randint(keys[3], (task_count,), 0, group_count), jnp.arange(task_count)].set(MOST)
    device = jnp.arange(device_count, dtype=jnp.int32)
    group = device // task_count
    task = device % task_count
    comp_targets = group[:, None] * task_count + jnp.arange(task_count, dtype=jnp.int32)[None, :]
    io_targets = jnp.arange(group_count, dtype=jnp.int32)[None, :] * task_count + task[:, None]
    near_targets = jnp.stack([group * task_count + (task + 1) % task_count, group * task_count + (task - 1) % task_count, (group + 1) % group_count * task_count + task, (group - 1) % group_count * task_count + task, device], axis=1)
    targets = jnp.concatenate([comp_targets, io_targets, near_targets], axis=1).astype(jnp.int32)
    spread_counts = jnp.full((device_count, task_count + group_count), SPREAD, jnp.int32)
    near_counts = jnp.stack([comp_pairs[group, task], comp_pairs[group, (task - 1) % task_count], io_pairs[group, task], io_pairs[(group - 1) % group_count, task]], axis=1).astype(jnp.int32)
    used = jnp.sum(spread_counts, axis=1) + jnp.sum(near_counts, axis=1)
    counts = jnp.concatenate([spread_counts, near_counts, (COLS_DEV - used)[:, None]], axis=1)
    ends = jnp.cumsum(counts, axis=1)
    position = jnp.arange(COLS_DEV, dtype=jnp.int32)
    segment = jax.vmap(lambda edge: jnp.searchsorted(edge, position, side='right'))(ends).astype(jnp.int32)
    owner = jnp.take_along_axis(targets, segment, axis=1)
    shuffles = jax.vmap(lambda k: jax.random.permutation(k, COLS_DEV))(jax.random.split(keys[4], device_count)).astype(jnp.int32)
    owner = jnp.take_along_axis(owner, shuffles, axis=1)
    flat_owner = owner.reshape(device_count * COLS_DEV)
    mixing = jax.random.permutation(keys[5], device_count * COLS_DEV).astype(jnp.int32)
    order = jnp.argsort(flat_owner[mixing], stable=True).astype(jnp.int32)
    offsets = jnp.zeros((device_count * COLS_DEV,), jnp.int32).at[mixing[order]].set(jnp.arange(device_count * COLS_DEV, dtype=jnp.int32))
    return offsets.reshape(device_count * COLS_DEV // 128, 128).astype(jnp.int32)


def shard_levels(rng, dims, cuts, low, largest):
    def one(axis_at, shards_of):
        steps = jax.random.uniform(jax.random.fold_in(jax.random.fold_in(rng, 6), axis_at), (shards_of,), jnp.float32, low / len(cuts), largest / len(cuts))
        return jnp.repeat(jnp.exp(steps), dims[axis_at] // shards_of).reshape((-1,) + (1,) * (len(dims) - axis_at - 1))

    factor_of = one(*cuts[0])
    for cut in cuts[1:]:
        factor_of = factor_of * one(*cut)
    return factor_of


def normal_values(key, extent, spread, reach, cuts=(), kind=jnp.bfloat16):
    entries = jax.random.normal(key, extent, jnp.float32) * spread
    if len(cuts) > 0:
        entries = shard_levels(key, extent, cuts, -0.22, 0.18) * entries
    return jnp.clip(entries, min=-reach, max=reach).astype(kind)


def setup_inputs(seed: int = 0) -> dict:
    streams_of = jax.random.split(jax.random.key(seed), 4)
    return {
        "fields": normal_values(streams_of[0], (COLS, FIELDS * LEV), 1.0, 6.0, ((0, 256),), jnp.float32),
        "file_offset": draw_file_offset(jax.random.fold_in(streams_of[3], 71), 0),
        "level_remap": normal_values(streams_of[2], (FIELDS, LEV, LEV), LEV ** -0.5, 0.75, (), jnp.float32),
    }


def reference(fields, file_offset, level_remap):
    columns = fields.shape[0]
    shaped = fields.reshape(columns, FIELDS, LEV)
    mixed = jnp.einsum("cfl,flm->cfm", shaped, level_remap, precision=lax.Precision.HIGHEST)
    remapped = mixed.reshape(columns, FIELDS * LEV)
    positions = file_offset.reshape(columns).astype(jnp.int32)
    history = jnp.zeros_like(remapped).at[positions].set(remapped)
    return history
```

```python
import jax
import jax.numpy as jnp
from jax import lax
from jax.experimental import pallas as pl
from jax.experimental.pallas import tpu as pltpu
from jax.sharding import PartitionSpec as P

SPREAD = 8
MOST = 192
COLUMNS = 3072
BLOCKS = COLUMNS // 128
WIDTH = 256
N_COMP = 64
N_IO = 4
PACKET = 2 * SPREAD + 1
NEAR_COMP = MOST
NEAR_IO = MOST + SPREAD
COMP_ROWS = 392
IO_ROWS = 408
FAR_ROWS = 24
KEYS = 80
DUMP = COLUMNS
PLACED = 2 * (COLUMNS + 8)
VMEM = pltpu.VMEM
SMEM = pltpu.SMEM


def coordinates():
    return lax.axis_index("io"), lax.axis_index("comp")


def pack_kernel(
    offsets_ref,
    fields_ref,
    spread_ref,
    up_ref,
    down_ref,
    next_ref,
    prev_ref,
    far_ref,
    stay_ref,
    fields,
    onehot,
    prefix,
    ranks,
    high,
    low,
    source,
    source_s,
    sems,
):
    fetch = pltpu.make_async_copy(fields_ref, fields, sems.at[0])
    fetch.start()
    group, task = coordinates()
    offset = offsets_ref[...]
    owner = ((offset >> 10) * 21846) >> 16
    position = offset - owner * COLUMNS
    owner_group = owner >> 6
    owner_task = owner & (N_COMP - 1)
    along_comp = (owner_group == group) & (owner_task != task)
    along_io = (owner_task == task) & (owner_group != group)
    key = jnp.where(along_comp, owner_task, jnp.where(along_io, N_COMP + owner_group, 127))
    rows = lax.broadcasted_iota(jnp.int32, (KEYS, 128), 0)
    for b in range(BLOCKS):
        hit = rows == key[b : b + 1, :]
        onehot[b * KEYS : (b + 1) * KEYS, :] = jnp.where(hit, 1.0, 0.0).astype(jnp.bfloat16)
    r = lax.broadcasted_iota(jnp.int32, (128, 256), 0)
    c = lax.broadcasted_iota(jnp.int32, (128, 256), 1)
    earlier = jnp.where((r < c) | (c >= 128), 1.0, 0.0).astype(jnp.bfloat16)
    prefix[...] = jnp.dot(onehot[...], earlier, preferred_element_type=jnp.float32)
    carry = jnp.zeros((KEYS, 128), jnp.float32)
    for b in range(BLOCKS):
        hit = rows == key[b : b + 1, :]
        counted = prefix[b * KEYS : (b + 1) * KEYS, 0:128] + carry
        ranks[b : b + 1, :] = jnp.sum(jnp.where(hit, counted, 0.0), axis=0, keepdims=True)
        carry = carry + prefix[b * KEYS : (b + 1) * KEYS, 128:256]
    rank = ranks[...].astype(jnp.int32)
    upper = (task + 1) & (N_COMP - 1)
    after = (group + 1) & (N_IO - 1)
    before = (group + N_IO - 1) & (N_IO - 1)
    comp_slot = jnp.where(
        rank < SPREAD,
        owner_task * SPREAD + rank,
        jnp.where(owner_task == upper, 512, 768) + rank - SPREAD,
    )
    io_slot = (
        jnp.where(owner_group == after, 1024, jnp.where(owner_group == before, 1280, 1536)) + rank
    )
    slot = jnp.where(along_comp, comp_slot, jnp.where(along_io, io_slot, 2047))
    stay_ref[...] = jnp.where(along_comp | along_io, DUMP, position)
    slot_high = slot >> 7
    slot_low = slot & 127
    column = lax.broadcasted_iota(jnp.int32, (BLOCKS, 128), 0) * 128 + lax.broadcasted_iota(
        jnp.int32, (BLOCKS, 128), 1
    )
    coded = position + 1
    parts = [
        (column & 255).astype(jnp.float32),
        (column >> 8).astype(jnp.float32),
        (coded & 255).astype(jnp.float32),
        (coded >> 8).astype(jnp.float32),
    ]
    rows16 = lax.broadcasted_iota(jnp.int32, (16, 128), 0)
    rows128 = lax.broadcasted_iota(jnp.int32, (128, 128), 0)
    for b in range(BLOCKS):
        hit = rows16 == slot_high[b : b + 1, :]
        for j in range(4):
            high[16 * j : 16 * (j + 1), 128 * b : 128 * (b + 1)] = jnp.where(
                hit, parts[j][b : b + 1, :], 0.0
            ).astype(jnp.bfloat16)
        low[:, 128 * b : 128 * (b + 1)] = jnp.where(
            rows128 == slot_low[b : b + 1, :], 1.0, 0.0
        ).astype(jnp.bfloat16)
    found = lax.dot_general(
        high[...], low[...], (((1,), (1,)), ((), ())), preferred_element_type=jnp.float32
    )
    chosen = (found[0:16, :] + 256.0 * found[16:32, :]).astype(jnp.int32)
    source[...] = (chosen >> 3) * 16 + (chosen & 7)
    push = pltpu.make_async_copy(source, source_s, sems.at[1])
    push.start()
    coded = found[32:48, :] + 256.0 * found[48:64, :]
    goal = jnp.where(coded > 0.5, coded - 1.0, float(DUMP))
    for t in range(N_COMP):
        spread_ref[PACKET * t + 2 * SPREAD : PACKET * (t + 1), :] = goal[t >> 4 : (t >> 4) + 1, :]
    up_ref[0:2, :] = goal[4:6, :]
    down_ref[0:2, :] = goal[6:8, :]
    next_ref[0:2, :] = goal[8:10, :]
    prev_ref[0:2, :] = goal[10:12, :]
    far_ref[0:1, :] = goal[12:13, :]
    push.wait()
    fetch.wait()

    def copy(into, at, row):
        into[pl.ds(at, 1), :] = fields[pl.ds(row, 1), :]
        into[pl.ds(at + 1, 1), :] = fields[pl.ds(row + 8, 1), :]

    def spread_step(i, _):
        for k in range(32):
            copy(spread_ref, i * (4 * PACKET) + (k // 8) * PACKET + 2 * (k % 8), source_s[i // 4, (i % 4) * 32 + k])
        return 0

    lax.fori_loop(0, 16, spread_step, 0)

    def near_step(into, base):
        def step(i, _):
            for k in range(8):
                copy(into, 2 + 16 * i + 2 * k, source_s[base + i // 16, (i % 16) * 8 + k])
            return 0

        return step

    lax.fori_loop(0, NEAR_COMP // 8, near_step(up_ref, 4), 0)
    lax.fori_loop(0, NEAR_COMP // 8, near_step(down_ref, 6), 0)
    lax.fori_loop(0, NEAR_IO // 8, near_step(next_ref, 8), 0)
    lax.fori_loop(0, NEAR_IO // 8, near_step(prev_ref, 10), 0)
    for k in range(SPREAD):
        copy(far_ref, 1 + 2 * k, source_s[12, k])


def local_kernel(stay_ref, fields_ref, remap_ref, placed_ref, high_ref, low_ref):
    zero = jnp.zeros((64, 64), jnp.float32)
    for f in range(4):
        band = jnp.concatenate([remap_ref[f] if g == f else zero for g in range(4)], axis=1)
        top = band.astype(jnp.bfloat16)
        high_ref[64 * f : 64 * (f + 1), :] = top
        low_ref[64 * f : 64 * (f + 1), :] = (band - top.astype(jnp.float32)).astype(jnp.bfloat16)

    def step(i, _):
        for k in range(16):
            at = 2 * stay_ref[i // 8, (i % 8) * 16 + k]
            row = 32 * i + 16 * (k // 8) + k % 8
            placed_ref[pl.ds(at, 1), :] = fields_ref[pl.ds(row, 1), :]
            placed_ref[pl.ds(at + 1, 1), :] = fields_ref[pl.ds(row + 8, 1), :]
        return 0

    lax.fori_loop(0, COLUMNS // 16, step, 0)


def final_kernel(
    spread_ref,
    up_ref,
    down_ref,
    next_ref,
    prev_ref,
    far_ref,
    placed_in,
    high_ref,
    low_ref,
    out_ref,
    placed,
    goal,
    goal_s,
    result,
    sems,
):
    fetch = pltpu.make_async_copy(placed_in, placed, sems.at[1])
    fetch.start()
    _, task = coordinates()
    for t in range(N_COMP):
        goal[t : t + 1, :] = spread_ref[PACKET * t + 2 * SPREAD : PACKET * (t + 1), :].astype(jnp.int32)
    for j, ref in enumerate((up_ref, down_ref, next_ref, prev_ref)):
        goal[64 + 2 * j : 66 + 2 * j, :] = ref[0:2, :].astype(jnp.int32)
    goal[72:73, :] = far_ref[0:1, :].astype(jnp.int32)
    push = pltpu.make_async_copy(goal, goal_s, sems.at[0])
    push.start()
    push.wait()
    fetch.wait()

    def copy(origin, at, row):
        to = 2 * row
        placed[pl.ds(to, 1), :] = origin[pl.ds(at, 1), :]
        placed[pl.ds(to + 1, 1), :] = origin[pl.ds(at + 1, 1), :]

    lane = (task & 15) * SPREAD

    def spread_step(i, _):
        for k in range(16):
            copy(spread_ref, i * (2 * PACKET) + (k // 8) * PACKET + 2 * (k % 8), goal_s[2 * i + k // 8, lane + k % 8])
        return 0

    lax.fori_loop(0, 32, spread_step, 0)

    def near_step(origin, base):
        def step(i, _):
            for k in range(8):
                copy(origin, 2 + 16 * i + 2 * k, goal_s[base + i // 16, (i % 16) * 8 + k])
            return 0

        return step

    lax.fori_loop(0, NEAR_COMP // 8, near_step(up_ref, 64), 0)
    lax.fori_loop(0, NEAR_COMP // 8, near_step(down_ref, 66), 0)
    lax.fori_loop(0, NEAR_IO // 8, near_step(next_ref, 68), 0)
    lax.fori_loop(0, NEAR_IO // 8, near_step(prev_ref, 70), 0)
    for k in range(SPREAD):
        copy(far_ref, 1 + 2 * k, goal_s[72, k])

    size = 512
    copies = []
    for j in range(COLUMNS // size):
        left = placed[pl.ds(2 * size * j, size, stride=2), :]
        right = placed[pl.ds(2 * size * j + 1, size, stride=2), :]
        x = jnp.concatenate([left, right], axis=1)
        x_high = x.astype(jnp.bfloat16)
        x_low = (x - x_high.astype(jnp.float32)).astype(jnp.bfloat16)
        total = jnp.dot(x_high, high_ref[...], preferred_element_type=jnp.float32)
        total += jnp.dot(x_high, low_ref[...], preferred_element_type=jnp.float32)
        total += jnp.dot(x_low, high_ref[...], preferred_element_type=jnp.float32)
        result[size * j : size * (j + 1), :] = total
        write = pltpu.make_async_copy(
            result.at[pl.ds(size * j, size), :],
            out_ref.at[pl.ds(size * j, size), :],
            sems.at[2 + j],
        )
        write.start()
        copies.append(write)
    for write in copies:
        write.wait()


def shift(value, axis, by):
    peers = lax.axis_size(axis)
    return lax.ppermute(value, axis, [(i, (i + by) % peers) for i in range(peers)])


def per_device(fields, file_offset, level_remap):
    f32 = jnp.float32
    whole = pl.BlockSpec(memory_space=VMEM)
    anywhere = pl.BlockSpec(memory_space=pl.ANY)
    scalars = pl.BlockSpec(memory_space=SMEM)
    fields = (
        fields.reshape(COLUMNS // 8, 8, 2, 128).transpose(0, 2, 1, 3).reshape(2 * COLUMNS, 128)
    )
    spread, up, down, after, before, far, stay = pl.pallas_call(
        pack_kernel,
        name="pack",
        out_shape=[
            jax.ShapeDtypeStruct((N_COMP * PACKET, 128), f32),
            jax.ShapeDtypeStruct((COMP_ROWS, 128), f32),
            jax.ShapeDtypeStruct((COMP_ROWS, 128), f32),
            jax.ShapeDtypeStruct((IO_ROWS, 128), f32),
            jax.ShapeDtypeStruct((IO_ROWS, 128), f32),
            jax.ShapeDtypeStruct((FAR_ROWS, 128), f32),
            jax.ShapeDtypeStruct((BLOCKS, 128), jnp.int32),
        ],
        in_specs=[whole, anywhere],
        out_specs=[whole] * 7,
        scratch_shapes=[
            VMEM((2 * COLUMNS, 128), f32),
            VMEM((BLOCKS * KEYS, 128), jnp.bfloat16),
            VMEM((BLOCKS * KEYS, 256), f32),
            VMEM((BLOCKS, 128), f32),
            VMEM((64, COLUMNS), jnp.bfloat16),
            VMEM((128, COLUMNS), jnp.bfloat16),
            VMEM((16, 128), jnp.int32),
            SMEM((16, 128), jnp.int32),
            pltpu.SemaphoreType.DMA((2,)),
        ],
        cost_estimate=pl.CostEstimate(flops=20_000_000, bytes_accessed=5_000_000, transcendentals=0),
    )(file_offset, fields)
    spread = lax.all_to_all(
        spread.reshape(N_COMP, 1, PACKET * 128), "comp", split_axis=0, concat_axis=0, tiled=True
    ).reshape(N_COMP * PACKET, 128)
    up = shift(up, "comp", 1)
    down = shift(down, "comp", -1)
    after = shift(after, "io", 1)
    before = shift(before, "io", -1)
    far = shift(far, "io", 2)
    placed, high, low = pl.pallas_call(
        local_kernel,
        name="local",
        out_shape=[
            jax.ShapeDtypeStruct((PLACED, 128), f32),
            jax.ShapeDtypeStruct((WIDTH, WIDTH), jnp.bfloat16),
            jax.ShapeDtypeStruct((WIDTH, WIDTH), jnp.bfloat16),
        ],
        in_specs=[scalars, whole, whole],
        out_specs=[whole] * 3,
        cost_estimate=pl.CostEstimate(flops=4_000_000_000, bytes_accessed=6_000_000, transcendentals=0),
    )(stay, fields, level_remap)
    return pl.pallas_call(
        final_kernel,
        name="final",
        out_shape=jax.ShapeDtypeStruct((COLUMNS, WIDTH), f32),
        in_specs=[whole] * 6 + [anywhere, whole, whole],
        out_specs=anywhere,
        scratch_shapes=[
            VMEM((PLACED, 128), f32),
            VMEM((80, 128), jnp.int32),
            SMEM((80, 128), jnp.int32),
            VMEM((COLUMNS, WIDTH), f32),
            pltpu.SemaphoreType.DMA((2 + COLUMNS // 512,)),
        ],
        cost_estimate=pl.CostEstimate(flops=1_000_000_000, bytes_accessed=8_000_000, transcendentals=0),
    )(spread, up, down, after, before, far, placed, high, low)


def solution(mesh):
    placed = (P(("io", "comp"), None), P(("io", "comp"), None), P())
    return jax.shard_map(
        per_device, mesh=mesh, in_specs=placed, out_specs=P(("io", "comp"), None), check_vma=False
    )
```

```python
import jax
import jax.numpy as jnp
from jax import lax
from jax.experimental import pallas as pl
from jax.experimental.pallas import tpu as pltpu
from jax.sharding import PartitionSpec as P


SPREAD = 8
MOST = 192
COLUMNS = 3072
BLOCKS = COLUMNS // 128
WIDTH = 256
N_COMP = 64
N_IO = 4
PACKET = 2 * SPREAD + 1
NEAR_COMP = MOST
NEAR_IO = MOST + SPREAD
COMP_ROWS = 392
IO_ROWS = 408
FAR_ROWS = 24
KEYS = 80
DUMP = COLUMNS
SIZES = (512, 512, 512, 512, 512, 256, 128, 128)
PLACED = 2 * (COLUMNS + 8)
VMEM = pltpu.VMEM
SMEM = pltpu.SMEM


def coordinates():
    return lax.axis_index("io"), lax.axis_index("comp")


def pack_kernel(
    offsets_ref,
    fields_ref,
    spread_out,
    up_ref,
    down_ref,
    next_ref,
    prev_ref,
    far_ref,
    stay_ref,
    fields,
    offsets,
    spread_ref,
    onehot,
    prefix,
    ranks,
    high,
    low,
    source,
    source_s,
    sems,
):
    fetch_offsets = pltpu.make_async_copy(offsets_ref, offsets, sems.at[2])
    fetch_offsets.start()
    fetch = pltpu.make_async_copy(fields_ref, fields, sems.at[0])
    fetch.start()
    fetch_offsets.wait()
    group, task = coordinates()
    offset = offsets[...]
    owner = ((offset >> 10) * 21846) >> 16
    position = offset - owner * COLUMNS
    owner_group = owner >> 6
    owner_task = owner & (N_COMP - 1)
    along_comp = (owner_group == group) & (owner_task != task)
    along_io = (owner_task == task) & (owner_group != group)
    key = jnp.where(along_comp, owner_task, jnp.where(along_io, N_COMP + owner_group, 127))
    rows = lax.broadcasted_iota(jnp.int32, (KEYS, 128), 0)
    for b in range(BLOCKS):
        hit = rows == key[b : b + 1, :]
        onehot[b * KEYS : (b + 1) * KEYS, :] = jnp.where(hit, 1.0, 0.0).astype(jnp.bfloat16)
    r = lax.broadcasted_iota(jnp.int32, (128, 256), 0)
    c = lax.broadcasted_iota(jnp.int32, (128, 256), 1)
    earlier = jnp.where((r < c) | (c >= 128), 1.0, 0.0).astype(jnp.bfloat16)
    prefix[...] = jnp.dot(onehot[...], earlier, preferred_element_type=jnp.float32)
    carry = jnp.zeros((KEYS, 128), jnp.float32)
    for b in range(BLOCKS):
        hit = rows == key[b : b + 1, :]
        counted = prefix[b * KEYS : (b + 1) * KEYS, 0:128] + carry
        ranks[b : b + 1, :] = jnp.sum(jnp.where(hit, counted, 0.0), axis=0, keepdims=True)
        carry = carry + prefix[b * KEYS : (b + 1) * KEYS, 128:256]
    rank = ranks[...].astype(jnp.int32)
    upper = (task + 1) & (N_COMP - 1)
    after = (group + 1) & (N_IO - 1)
    before = (group + N_IO - 1) & (N_IO - 1)
    comp_slot = jnp.where(
        rank < SPREAD,
        owner_task * SPREAD + rank,
        jnp.where(owner_task == upper, 512, 768) + rank - SPREAD,
    )
    io_slot = (
        jnp.where(owner_group == after, 1024, jnp.where(owner_group == before, 1280, 1536)) + rank
    )
    slot = jnp.where(along_comp, comp_slot, jnp.where(along_io, io_slot, 2047))
    stay_ref[...] = 2 * jnp.where(along_comp | along_io, DUMP, position)
    slot_high = slot >> 7
    slot_low = slot & 127
    column = lax.broadcasted_iota(jnp.int32, (BLOCKS, 128), 0) * 128 + lax.broadcasted_iota(
        jnp.int32, (BLOCKS, 128), 1
    )
    coded = position + 1
    parts = [
        (column & 255).astype(jnp.float32),
        (column >> 8).astype(jnp.float32),
        (coded & 255).astype(jnp.float32),
        (coded >> 8).astype(jnp.float32),
    ]
    rows16 = lax.broadcasted_iota(jnp.int32, (16, 128), 0)
    rows128 = lax.broadcasted_iota(jnp.int32, (128, 128), 0)
    for b in range(BLOCKS):
        hit = rows16 == slot_high[b : b + 1, :]
        for j in range(4):
            high[16 * j : 16 * (j + 1), 128 * b : 128 * (b + 1)] = jnp.where(
                hit, parts[j][b : b + 1, :], 0.0
            ).astype(jnp.bfloat16)
        low[:, 128 * b : 128 * (b + 1)] = jnp.where(
            rows128 == slot_low[b : b + 1, :], 1.0, 0.0
        ).astype(jnp.bfloat16)
    found = lax.dot_general(
        high[...], low[...], (((1,), (1,)), ((), ())), preferred_element_type=jnp.float32
    )
    chosen = (found[0:16, :] + 256.0 * found[16:32, :]).astype(jnp.int32)
    source[...] = (chosen >> 3) * 16 + (chosen & 7)
    push = pltpu.make_async_copy(source, source_s, sems.at[1])
    push.start()
    coded = found[32:48, :] + 256.0 * found[48:64, :]
    goal = 2.0 * jnp.where(coded > 0.5, coded - 1.0, float(DUMP))
    turned = pltpu.roll(goal, (task & 15) * SPREAD, 1)
    for j in range(16):
        row = pltpu.roll(turned, (128 - SPREAD * j) % 128, 1)
        for g in range(N_COMP // 16):
            at = PACKET * (16 * g + j) + 2 * SPREAD
            spread_ref[at : at + 1, :] = row[g : g + 1, :]
    up_ref[0:2, :] = goal[4:6, :]
    down_ref[0:2, :] = goal[6:8, :]
    next_ref[0:2, :] = goal[8:10, :]
    prev_ref[0:2, :] = goal[10:12, :]
    far_ref[0:1, :] = goal[12:13, :]
    push.wait()
    fetch.wait()

    def copy(into, at, slot):
        row = source_s[slot // 128, slot % 128]
        into[pl.ds(at, 1), :] = fields[pl.ds(row, 1), :]
        into[pl.ds(at + 1, 1), :] = fields[pl.ds(row + 8, 1), :]

    part = N_COMP * PACKET // 4
    writes = []
    for q in range(4):
        for s in range(128 * q, 128 * (q + 1)):
            copy(spread_ref, PACKET * (s // SPREAD) + 2 * (s % SPREAD), s)
        write = pltpu.make_async_copy(
            spread_ref.at[pl.ds(part * q, part), :],
            spread_out.at[pl.ds(part * q, part), :],
            sems.at[3 + q],
        )
        write.start()
        writes.append(write)
    for s in range(NEAR_COMP):
        copy(up_ref, 2 + 2 * s, 512 + s)
    for s in range(NEAR_COMP):
        copy(down_ref, 2 + 2 * s, 768 + s)
    for s in range(NEAR_IO):
        copy(next_ref, 2 + 2 * s, 1024 + s)
    for s in range(NEAR_IO):
        copy(prev_ref, 2 + 2 * s, 1280 + s)
    for s in range(SPREAD):
        copy(far_ref, 1 + 2 * s, 1536 + s)
    for write in writes:
        write.wait()


def local_kernel(stay_ref, fields_in, remap_ref, placed_ref, high_ref, low_ref, fields_ref, sems):
    part = 2 * COLUMNS // 4
    fetches = []
    for q in range(4):
        fetch = pltpu.make_async_copy(
            fields_in.at[pl.ds(part * q, part), :],
            fields_ref.at[pl.ds(part * q, part), :],
            sems.at[q],
        )
        fetch.start()
        fetches.append(fetch)
    zero = jnp.zeros((64, 64), jnp.float32)
    for f in range(4):
        band = jnp.concatenate([remap_ref[f] if g == f else zero for g in range(4)], axis=1)
        top = band.astype(jnp.bfloat16)
        high_ref[64 * f : 64 * (f + 1), :] = top
        low_ref[64 * f : 64 * (f + 1), :] = (band - top.astype(jnp.float32)).astype(jnp.bfloat16)

    def step(i, _):
        for k in range(128):
            at = stay_ref[i, k]
            row = 256 * i + 16 * (k // 8) + k % 8
            placed_ref[pl.ds(at, 1), :] = fields_ref[pl.ds(row, 1), :]
            placed_ref[pl.ds(at + 1, 1), :] = fields_ref[pl.ds(row + 8, 1), :]
        return 0

    for q, fetch in enumerate(fetches):
        fetch.wait()
        lax.fori_loop(BLOCKS // 4 * q, BLOCKS // 4 * (q + 1), step, 0)


def final_kernel(
    spread_ref,
    up_ref,
    down_ref,
    next_ref,
    prev_ref,
    far_ref,
    placed_in,
    high_ref,
    low_ref,
    out_ref,
    placed,
    goal,
    goal_s,
    result,
    sems,
):
    fetch = pltpu.make_async_copy(placed_in, placed, sems.at[1])
    fetch.start()
    rows = jnp.concatenate(
        [spread_ref[PACKET * t + 2 * SPREAD : PACKET * (t + 1), :] for t in range(N_COMP)], axis=0
    )
    packet = lax.broadcasted_iota(jnp.int32, (N_COMP, 128), 0)
    lane = lax.broadcasted_iota(jnp.int32, (N_COMP, 128), 1)
    rows = jnp.where((packet & 15) == (lane >> 3), rows, 0.0)
    goal[0:4, :] = jnp.sum(rows.reshape(4, 16, 128), axis=1).astype(jnp.int32)
    for j, ref in enumerate((up_ref, down_ref, next_ref, prev_ref)):
        goal[4 + 2 * j : 6 + 2 * j, :] = ref[0:2, :].astype(jnp.int32)
    goal[12:13, :] = far_ref[0:1, :].astype(jnp.int32)
    push = pltpu.make_async_copy(goal, goal_s, sems.at[0])
    push.start()
    push.wait()
    fetch.wait()

    def copy(origin, at, slot):
        to = goal_s[slot // 128, slot % 128]
        placed[pl.ds(to, 1), :] = origin[pl.ds(at, 1), :]
        placed[pl.ds(to + 1, 1), :] = origin[pl.ds(at + 1, 1), :]

    for s in range(N_COMP * SPREAD):
        copy(spread_ref, PACKET * (s // SPREAD) + 2 * (s % SPREAD), s)
    for s in range(NEAR_COMP):
        copy(up_ref, 2 + 2 * s, 512 + s)
    for s in range(NEAR_COMP):
        copy(down_ref, 2 + 2 * s, 768 + s)
    for s in range(NEAR_IO):
        copy(next_ref, 2 + 2 * s, 1024 + s)
    for s in range(NEAR_IO):
        copy(prev_ref, 2 + 2 * s, 1280 + s)
    for s in range(SPREAD):
        copy(far_ref, 1 + 2 * s, 1536 + s)

    copies = []
    start = 0
    for j, size in enumerate(SIZES):
        left = placed[pl.ds(2 * start, size, stride=2), :]
        right = placed[pl.ds(2 * start + 1, size, stride=2), :]
        x = jnp.concatenate([left, right], axis=1)
        x_high = x.astype(jnp.bfloat16)
        x_low = (x - x_high.astype(jnp.float32)).astype(jnp.bfloat16)
        total = jnp.dot(x_high, high_ref[...], preferred_element_type=jnp.float32)
        total += jnp.dot(x_high, low_ref[...], preferred_element_type=jnp.float32)
        total += jnp.dot(x_low, high_ref[...], preferred_element_type=jnp.float32)
        result[start : start + size, :] = total
        write = pltpu.make_async_copy(
            result.at[pl.ds(start, size), :], out_ref.at[pl.ds(start, size), :], sems.at[2 + j]
        )
        write.start()
        copies.append(write)
        start += size
    for write in copies:
        write.wait()


def shift(value, axis, by):
    peers = lax.axis_size(axis)
    return lax.ppermute(value, axis, [(i, (i + by) % peers) for i in range(peers)])


def per_device(fields, file_offset, level_remap):
    f32 = jnp.float32
    whole = pl.BlockSpec(memory_space=VMEM)
    anywhere = pl.BlockSpec(memory_space=pl.ANY)
    scalars = pl.BlockSpec(memory_space=SMEM)
    fields = (
        fields.reshape(COLUMNS // 8, 8, 2, 128).transpose(0, 2, 1, 3).reshape(2 * COLUMNS, 128)
    )
    fields = pltpu.with_memory_space_constraint(fields, pltpu.HBM)
    file_offset = pltpu.with_memory_space_constraint(file_offset, pltpu.HBM)
    spread, up, down, after, before, far, stay = pl.pallas_call(
        pack_kernel,
        name="pack",
        out_shape=[
            pltpu.HBM((N_COMP * PACKET, 128), f32),
            VMEM((COMP_ROWS, 128), f32),
            VMEM((COMP_ROWS, 128), f32),
            VMEM((IO_ROWS, 128), f32),
            VMEM((IO_ROWS, 128), f32),
            VMEM((FAR_ROWS, 128), f32),
            pltpu.HBM((BLOCKS, 128), jnp.int32),
        ],
        in_specs=[anywhere, anywhere],
        out_specs=[anywhere] + [whole] * 6,
        scratch_shapes=[
            VMEM((2 * COLUMNS, 128), f32),
            VMEM((BLOCKS, 128), jnp.int32),
            VMEM((N_COMP * PACKET, 128), f32),
            VMEM((BLOCKS * KEYS, 128), jnp.bfloat16),
            VMEM((BLOCKS * KEYS, 256), f32),
            VMEM((BLOCKS, 128), f32),
            VMEM((64, COLUMNS), jnp.bfloat16),
            VMEM((128, COLUMNS), jnp.bfloat16),
            VMEM((16, 128), jnp.int32),
            SMEM((16, 128), jnp.int32),
            pltpu.SemaphoreType.DMA((7,)),
        ],
        compiler_params=pltpu.CompilerParams(vmem_limit_bytes=40 * 2**20),
        cost_estimate=pl.CostEstimate(flops=20_000_000, bytes_accessed=5_000_000, transcendentals=0),
    )(file_offset, fields)
    spread = lax.all_to_all(
        spread.reshape(N_COMP, 1, PACKET * 128), "comp", split_axis=0, concat_axis=0, tiled=True
    ).reshape(N_COMP * PACKET, 128)
    up = shift(up, "comp", 1)
    down = shift(down, "comp", -1)
    after = shift(after, "io", 1)
    before = shift(before, "io", -1)
    far = shift(far, "io", 2)
    placed, high, low = pl.pallas_call(
        local_kernel,
        name="local",
        out_shape=[
            pltpu.HBM((PLACED, 128), f32),
            VMEM((WIDTH, WIDTH), jnp.bfloat16),
            VMEM((WIDTH, WIDTH), jnp.bfloat16),
        ],
        in_specs=[scalars, anywhere, whole],
        out_specs=[whole] * 3,
        scratch_shapes=[VMEM((2 * COLUMNS, 128), f32), pltpu.SemaphoreType.DMA((4,))],
        compiler_params=pltpu.CompilerParams(vmem_limit_bytes=40 * 2**20),
        cost_estimate=pl.CostEstimate(flops=4_000_000_000, bytes_accessed=6_000_000, transcendentals=0),
    )(stay, fields, level_remap)
    operands = [
        pltpu.with_memory_space_constraint(x, VMEM)
        for x in (spread, up, down, after, before, far, high, low)
    ]
    operands.insert(6, pltpu.with_memory_space_constraint(placed, pltpu.HBM))
    return pl.pallas_call(
        final_kernel,
        name="final",
        out_shape=jax.ShapeDtypeStruct((COLUMNS, WIDTH), f32),
        in_specs=[whole] * 6 + [anywhere, whole, whole],
        out_specs=anywhere,
        scratch_shapes=[
            VMEM((PLACED, 128), f32),
            VMEM((16, 128), jnp.int32),
            SMEM((16, 128), jnp.int32),
            VMEM((COLUMNS, WIDTH), f32),
            pltpu.SemaphoreType.DMA((2 + len(SIZES),)),
        ],
        compiler_params=pltpu.CompilerParams(vmem_limit_bytes=40 * 2**20),
        cost_estimate=pl.CostEstimate(flops=1_000_000_000, bytes_accessed=8_000_000, transcendentals=0),
    )(*operands)


def solution(mesh):
    placed = (P(("io", "comp"), None), P(("io", "comp"), None), P())

    return jax.shard_map(
        per_device, mesh=mesh, in_specs=placed, out_specs=P(("io", "comp"), None), check_vma=False
    )
```

```python
import jax
import jax.numpy as jnp
from jax import lax
from jax.experimental import pallas as pl
from jax.experimental.pallas import tpu as pltpu
from jax.sharding import PartitionSpec as P


SPREAD = 8
MOST = 192
COLUMNS = 3072
BLOCKS = COLUMNS // 128
WIDTH = 256
N_COMP = 64
N_IO = 4
PACKET = 2 * SPREAD + 1
NEAR_COMP = MOST
NEAR_IO = MOST + SPREAD
COMP_ROWS = 392
IO_ROWS = 408
FAR_ROWS = 24
KEYS = 80
DUMP = COLUMNS
RECEIVED = N_COMP * SPREAD + 2 * NEAR_COMP + 2 * NEAR_IO + SPREAD
PLACED = 2 * (COLUMNS + 8)
VMEM = pltpu.VMEM
SMEM = pltpu.SMEM


def coordinates():
    return lax.axis_index("io"), lax.axis_index("comp")


def pack_kernel(
    offsets_ref,
    fields_ref,
    spread_out,
    up_ref,
    down_ref,
    next_ref,
    prev_ref,
    far_ref,
    stay_ref,
    fields,
    offsets,
    spread_ref,
    onehot,
    prefix,
    ranks,
    high,
    low,
    source,
    source_s,
    sems,
):
    fetch_offsets = pltpu.make_async_copy(offsets_ref, offsets, sems.at[2])
    fetch_offsets.start()
    fetch = pltpu.make_async_copy(fields_ref, fields, sems.at[0])
    fetch.start()
    fetch_offsets.wait()
    group, task = coordinates()
    offset = offsets[...]
    owner = ((offset >> 10) * 21846) >> 16
    position = offset - owner * COLUMNS
    owner_group = owner >> 6
    owner_task = owner & (N_COMP - 1)
    along_comp = (owner_group == group) & (owner_task != task)
    along_io = (owner_task == task) & (owner_group != group)
    key = jnp.where(along_comp, owner_task, jnp.where(along_io, N_COMP + owner_group, 127))
    rows = lax.broadcasted_iota(jnp.int32, (KEYS, 128), 0)
    for b in range(BLOCKS):
        hit = rows == key[b : b + 1, :]
        onehot[b * KEYS : (b + 1) * KEYS, :] = jnp.where(hit, 1.0, 0.0).astype(jnp.bfloat16)
    r = lax.broadcasted_iota(jnp.int32, (128, 256), 0)
    c = lax.broadcasted_iota(jnp.int32, (128, 256), 1)
    earlier = jnp.where((r < c) | (c >= 128), 1.0, 0.0).astype(jnp.bfloat16)
    prefix[...] = jnp.dot(onehot[...], earlier, preferred_element_type=jnp.float32)
    carry = jnp.zeros((KEYS, 128), jnp.float32)
    for b in range(BLOCKS):
        hit = rows == key[b : b + 1, :]
        counted = prefix[b * KEYS : (b + 1) * KEYS, 0:128] + carry
        ranks[b : b + 1, :] = jnp.sum(jnp.where(hit, counted, 0.0), axis=0, keepdims=True)
        carry = carry + prefix[b * KEYS : (b + 1) * KEYS, 128:256]
    rank = ranks[...].astype(jnp.int32)
    upper = (task + 1) & (N_COMP - 1)
    after = (group + 1) & (N_IO - 1)
    before = (group + N_IO - 1) & (N_IO - 1)
    comp_slot = jnp.where(
        rank < SPREAD,
        owner_task * SPREAD + rank,
        jnp.where(owner_task == upper, 512, 768) + rank - SPREAD,
    )
    io_slot = (
        jnp.where(owner_group == after, 1024, jnp.where(owner_group == before, 1280, 1536)) + rank
    )
    slot = jnp.where(along_comp, comp_slot, jnp.where(along_io, io_slot, 2047))
    stay_ref[...] = 2 * jnp.where(along_comp | along_io, DUMP, position)
    slot_high = slot >> 7
    slot_low = slot & 127
    column = lax.broadcasted_iota(jnp.int32, (BLOCKS, 128), 0) * 128 + lax.broadcasted_iota(
        jnp.int32, (BLOCKS, 128), 1
    )
    coded = position + 1
    parts = [
        (column & 255).astype(jnp.float32),
        (column >> 8).astype(jnp.float32),
        (coded & 255).astype(jnp.float32),
        (coded >> 8).astype(jnp.float32),
    ]
    rows16 = lax.broadcasted_iota(jnp.int32, (16, 128), 0)
    rows128 = lax.broadcasted_iota(jnp.int32, (128, 128), 0)
    for b in range(BLOCKS):
        hit = rows16 == slot_high[b : b + 1, :]
        for j in range(4):
            high[16 * j : 16 * (j + 1), 128 * b : 128 * (b + 1)] = jnp.where(
                hit, parts[j][b : b + 1, :], 0.0
            ).astype(jnp.bfloat16)
        low[:, 128 * b : 128 * (b + 1)] = jnp.where(
            rows128 == slot_low[b : b + 1, :], 1.0, 0.0
        ).astype(jnp.bfloat16)
    found = lax.dot_general(
        high[...], low[...], (((1,), (1,)), ((), ())), preferred_element_type=jnp.float32
    )
    chosen = (found[0:16, :] + 256.0 * found[16:32, :]).astype(jnp.int32)
    source[...] = (chosen >> 3) * 16 + (chosen & 7)
    push = pltpu.make_async_copy(source, source_s, sems.at[1])
    push.start()
    coded = found[32:48, :] + 256.0 * found[48:64, :]
    goal = jnp.where(coded > 0.5, coded - 1.0, float(DUMP)).astype(jnp.int32)
    goal = ((goal >> 3) * 16 + (goal & 7)).astype(jnp.float32)
    turned = pltpu.roll(goal, (task & 15) * SPREAD, 1)
    for j in range(16):
        row = pltpu.roll(turned, (128 - SPREAD * j) % 128, 1)
        for g in range(N_COMP // 16):
            at = PACKET * (16 * g + j) + 2 * SPREAD
            spread_ref[at : at + 1, :] = row[g : g + 1, :]
    up_ref[0:2, :] = goal[4:6, :]
    down_ref[0:2, :] = goal[6:8, :]
    next_ref[0:2, :] = goal[8:10, :]
    prev_ref[0:2, :] = goal[10:12, :]
    far_ref[0:1, :] = goal[12:13, :]
    push.wait()
    fetch.wait()

    def copy(into, at, slot):
        row = source_s[slot // 128, slot % 128]
        into[pl.ds(at, 2), :] = fields[pl.ds(row, 2, stride=8), :]

    part = N_COMP * PACKET // 4
    writes = []
    for q in range(4):
        for s in range(128 * q, 128 * (q + 1)):
            copy(spread_ref, PACKET * (s // SPREAD) + 2 * (s % SPREAD), s)
        write = pltpu.make_async_copy(
            spread_ref.at[pl.ds(part * q, part), :],
            spread_out.at[pl.ds(part * q, part), :],
            sems.at[3 + q],
        )
        write.start()
        writes.append(write)
    for s in range(NEAR_COMP):
        copy(up_ref, 2 + 2 * s, 512 + s)
    for s in range(NEAR_COMP):
        copy(down_ref, 2 + 2 * s, 768 + s)
    for s in range(NEAR_IO):
        copy(next_ref, 2 + 2 * s, 1024 + s)
    for s in range(NEAR_IO):
        copy(prev_ref, 2 + 2 * s, 1280 + s)
    for s in range(SPREAD):
        copy(far_ref, 1 + 2 * s, 1536 + s)
    for write in writes:
        write.wait()


def remap(x, high_ref, low_ref):
    x_high = x.astype(jnp.bfloat16)
    x_low = (x - x_high.astype(jnp.float32)).astype(jnp.bfloat16)
    total = jnp.dot(x_high, high_ref[...], preferred_element_type=jnp.float32)
    total += jnp.dot(x_high, low_ref[...], preferred_element_type=jnp.float32)
    total += jnp.dot(x_low, high_ref[...], preferred_element_type=jnp.float32)
    return total


def local_kernel(
    stay_in, fields_in, remap_ref, kept_ref, high_ref, low_ref, fields, placed, result, stay, sems
):
    fetch_stay = pltpu.make_async_copy(stay_in, stay, sems.at[4])
    fetch_stay.start()
    part = 2 * COLUMNS // 4
    fetches = []
    for q in range(4):
        fetch = pltpu.make_async_copy(
            fields_in.at[pl.ds(part * q, part), :],
            fields.at[pl.ds(part * q, part), :],
            sems.at[q],
        )
        fetch.start()
        fetches.append(fetch)
    zero = jnp.zeros((64, 64), jnp.float32)
    for f in range(4):
        band = jnp.concatenate([remap_ref[f] if g == f else zero for g in range(4)], axis=1)
        top = band.astype(jnp.bfloat16)
        high_ref[64 * f : 64 * (f + 1), :] = top
        low_ref[64 * f : 64 * (f + 1), :] = (band - top.astype(jnp.float32)).astype(jnp.bfloat16)
    fetch_stay.wait()
    for q, fetch in enumerate(fetches):
        fetch.wait()
        for c in range(COLUMNS // 4 * q, COLUMNS // 4 * (q + 1)):
            row = 16 * (c // 8) + c % 8
            placed[pl.ds(stay[c // 128, c % 128], 2), :] = fields[pl.ds(row, 2, stride=8), :]
    writes = []
    size = 512
    for j in range(COLUMNS // size):
        left = placed[pl.ds(2 * size * j, size, stride=2), :]
        right = placed[pl.ds(2 * size * j + 1, size, stride=2), :]
        result[size * j : size * (j + 1), :] = remap(
            jnp.concatenate([left, right], axis=1), high_ref, low_ref
        )
        write = pltpu.make_async_copy(
            result.at[pl.ds(size * j, size), :],
            kept_ref.at[pl.ds(size * j, size), :],
            sems.at[5 + j],
        )
        write.start()
        writes.append(write)
    for write in writes:
        write.wait()


def final_kernel(
    spread_ref,
    up_ref,
    down_ref,
    next_ref,
    prev_ref,
    far_ref,
    kept_in,
    high_ref,
    low_ref,
    out_ref,
    kept,
    goal,
    goal_s,
    mixed,
    sems,
):
    part = 2 * COLUMNS // 4
    fetches = []
    for q in range(4):
        fetch = pltpu.make_async_copy(
            kept_in.at[pl.ds(part * q, part), :], kept.at[pl.ds(part * q, part), :], sems.at[1 + q]
        )
        fetch.start()
        fetches.append(fetch)
    rows = jnp.concatenate(
        [spread_ref[PACKET * t + 2 * SPREAD : PACKET * (t + 1), :] for t in range(N_COMP)], axis=0
    )
    packet = lax.broadcasted_iota(jnp.int32, (N_COMP, 128), 0)
    lane = lax.broadcasted_iota(jnp.int32, (N_COMP, 128), 1)
    rows = jnp.where((packet & 15) == (lane >> 3), rows, 0.0)
    goal[0:4, :] = jnp.sum(rows.reshape(4, 16, 128), axis=1).astype(jnp.int32)
    for j, ref in enumerate((up_ref, down_ref, next_ref, prev_ref)):
        goal[4 + 2 * j : 6 + 2 * j, :] = ref[0:2, :].astype(jnp.int32)
    goal[12:13, :] = far_ref[0:1, :].astype(jnp.int32)
    push = pltpu.make_async_copy(goal, goal_s, sems.at[0])
    push.start()

    def halves(ref, first, count, stride, step):
        return jnp.concatenate(
            [ref[pl.ds(first, count, stride=stride), :], ref[pl.ds(first + step, count, stride=stride), :]],
            axis=1,
        )

    groups = [
        [halves(spread_ref, 2 * k, N_COMP, PACKET, 1) for k in range(SPREAD)],
        [halves(ref, 2, NEAR_COMP, 2, 1) for ref in (up_ref, down_ref)],
        [halves(ref, 2, NEAR_IO, 2, 1) for ref in (next_ref, prev_ref)]
        + [halves(far_ref, 1, SPREAD, 2, 1)],
    ]
    at = 0
    for group in groups:
        total = remap(jnp.concatenate(group, axis=0), high_ref, low_ref)
        for g in range(total.shape[0] // 8):
            mixed[at : at + 8, :] = total[8 * g : 8 * (g + 1), 0:128]
            mixed[at + 8 : at + 16, :] = total[8 * g : 8 * (g + 1), 128:256]
            at += 16
    push.wait()
    for fetch in fetches:
        fetch.wait()

    def copy(row, slot):
        kept[pl.ds(goal_s[slot // 128, slot % 128], 2, stride=8), :] = mixed[
            pl.ds(16 * (row // 8) + row % 8, 2, stride=8), :
        ]

    for s in range(N_COMP * SPREAD):
        copy(N_COMP * (s % SPREAD) + s // SPREAD, s)
    row = N_COMP * SPREAD
    for base, count in ((512, NEAR_COMP), (768, NEAR_COMP), (1024, NEAR_IO), (1280, NEAR_IO), (1536, SPREAD)):
        for s in range(count):
            copy(row + s, base + s)
        row += count
    writes = []
    for q in range(4):
        write = pltpu.make_async_copy(
            kept.at[pl.ds(part * q, part), :], out_ref.at[pl.ds(part * q, part), :], sems.at[1 + q]
        )
        write.start()
        writes.append(write)
    for write in writes:
        write.wait()


def shift(value, axis, by):
    peers = lax.axis_size(axis)
    return lax.ppermute(value, axis, [(i, (i + by) % peers) for i in range(peers)])


def per_device(fields, file_offset, level_remap):
    f32 = jnp.float32
    whole = pl.BlockSpec(memory_space=VMEM)
    anywhere = pl.BlockSpec(memory_space=pl.ANY)
    fields = (
        fields.reshape(COLUMNS // 8, 8, 2, 128).transpose(0, 2, 1, 3).reshape(2 * COLUMNS, 128)
    )
    fields = pltpu.with_memory_space_constraint(fields, pltpu.HBM)
    file_offset = pltpu.with_memory_space_constraint(file_offset, pltpu.HBM)
    spread, up, down, after, before, far, stay = pl.pallas_call(
        pack_kernel,
        name="pack",
        out_shape=[
            pltpu.HBM((N_COMP * PACKET, 128), f32),
            VMEM((COMP_ROWS, 128), f32),
            VMEM((COMP_ROWS, 128), f32),
            VMEM((IO_ROWS, 128), f32),
            VMEM((IO_ROWS, 128), f32),
            VMEM((FAR_ROWS, 128), f32),
            pltpu.HBM((BLOCKS, 128), jnp.int32),
        ],
        in_specs=[anywhere, anywhere],
        out_specs=[anywhere] + [whole] * 6,
        scratch_shapes=[
            VMEM((2 * COLUMNS, 128), f32),
            VMEM((BLOCKS, 128), jnp.int32),
            VMEM((N_COMP * PACKET, 128), f32),
            VMEM((BLOCKS * KEYS, 128), jnp.bfloat16),
            VMEM((BLOCKS * KEYS, 256), f32),
            VMEM((BLOCKS, 128), f32),
            VMEM((64, COLUMNS), jnp.bfloat16),
            VMEM((128, COLUMNS), jnp.bfloat16),
            VMEM((16, 128), jnp.int32),
            SMEM((16, 128), jnp.int32),
            pltpu.SemaphoreType.DMA((7,)),
        ],
        compiler_params=pltpu.CompilerParams(vmem_limit_bytes=40 * 2**20),
        cost_estimate=pl.CostEstimate(flops=20_000_000, bytes_accessed=5_000_000, transcendentals=0),
    )(file_offset, fields)
    spread = lax.all_to_all(
        spread.reshape(N_COMP, 1, PACKET * 128), "comp", split_axis=0, concat_axis=0, tiled=True
    ).reshape(N_COMP * PACKET, 128)
    up = shift(up, "comp", 1)
    down = shift(down, "comp", -1)
    after = shift(after, "io", 1)
    before = shift(before, "io", -1)
    far = shift(far, "io", 2)
    kept, high, low = pl.pallas_call(
        local_kernel,
        name="local",
        out_shape=[
            pltpu.HBM((COLUMNS, WIDTH), f32),
            VMEM((WIDTH, WIDTH), jnp.bfloat16),
            VMEM((WIDTH, WIDTH), jnp.bfloat16),
        ],
        in_specs=[anywhere, anywhere, whole],
        out_specs=[anywhere, whole, whole],
        scratch_shapes=[
            VMEM((2 * COLUMNS, 128), f32),
            VMEM((PLACED, 128), f32),
            VMEM((COLUMNS, WIDTH), f32),
            SMEM((BLOCKS, 128), jnp.int32),
            pltpu.SemaphoreType.DMA((5 + COLUMNS // 512,)),
        ],
        compiler_params=pltpu.CompilerParams(vmem_limit_bytes=40 * 2**20),
        cost_estimate=pl.CostEstimate(flops=4_000_000_000, bytes_accessed=6_000_000, transcendentals=0),
    )(pltpu.with_memory_space_constraint(stay, pltpu.HBM), fields, level_remap)
    kept = kept.reshape(COLUMNS // 8, 8, 2, 128).transpose(0, 2, 1, 3).reshape(2 * COLUMNS, 128)
    operands = [
        pltpu.with_memory_space_constraint(x, VMEM)
        for x in (spread, up, down, after, before, far, high, low)
    ]
    operands.insert(6, pltpu.with_memory_space_constraint(kept, pltpu.HBM))
    out = pl.pallas_call(
        final_kernel,
        name="final",
        out_shape=jax.ShapeDtypeStruct((2 * COLUMNS, 128), f32),
        in_specs=[whole] * 6 + [anywhere, whole, whole],
        out_specs=anywhere,
        scratch_shapes=[
            VMEM((PLACED, 128), f32),
            VMEM((16, 128), jnp.int32),
            SMEM((16, 128), jnp.int32),
            VMEM((2 * RECEIVED, 128), f32),
            pltpu.SemaphoreType.DMA((5,)),
        ],
        compiler_params=pltpu.CompilerParams(vmem_limit_bytes=40 * 2**20),
        cost_estimate=pl.CostEstimate(flops=1_000_000_000, bytes_accessed=8_000_000, transcendentals=0),
    )(*operands)
    return out.reshape(COLUMNS // 8, 2, 8, 128).transpose(0, 2, 1, 3).reshape(COLUMNS, WIDTH)


def solution(mesh):
    placed = (P(("io", "comp"), None), P(("io", "comp"), None), P())

    return jax.shard_map(
        per_device, mesh=mesh, in_specs=placed, out_specs=P(("io", "comp"), None), check_vma=False
    )
```

```python
import jax
import jax.numpy as jnp
from jax import lax
from jax.experimental import pallas as pl
from jax.experimental.pallas import tpu as pltpu
from jax.sharding import PartitionSpec as P


SPREAD = 8
MOST = 192
COLUMNS = 3072
BLOCKS = COLUMNS // 128
WIDTH = 256
N_COMP = 64
N_IO = 4
PACKET = 2 * SPREAD + 1
NEAR_COMP = MOST
NEAR_IO = MOST + SPREAD
COMP_ROWS = 392
IO_ROWS = 408
FAR_ROWS = 24
KEYS = 80
DUMP = COLUMNS
RECEIVED = N_COMP * SPREAD + 2 * NEAR_COMP + 2 * NEAR_IO + SPREAD
PLACED = 2 * (COLUMNS + 8)
VMEM = pltpu.VMEM
SMEM = pltpu.SMEM


def coordinates():
    return lax.axis_index("io"), lax.axis_index("comp")


def pack_kernel(
    offsets_ref,
    fields_ref,
    spread_out,
    up_ref,
    down_ref,
    next_ref,
    prev_ref,
    far_ref,
    stay_out,
    fields,
    offsets,
    stay_ref,
    spread_ref,
    onehot,
    prefix,
    ranks,
    high,
    low,
    source,
    source_s,
    sems,
):
    fetch_offsets = pltpu.make_async_copy(offsets_ref, offsets, sems.at[2])
    fetch_offsets.start()
    fetch = pltpu.make_async_copy(fields_ref, fields, sems.at[0])
    fetch.start()
    fetch_offsets.wait()
    group, task = coordinates()
    offset = offsets[...]
    owner = ((offset >> 10) * 21846) >> 16
    position = offset - owner * COLUMNS
    owner_group = owner >> 6
    owner_task = owner & (N_COMP - 1)
    along_comp = (owner_group == group) & (owner_task != task)
    along_io = (owner_task == task) & (owner_group != group)
    key = jnp.where(along_comp, owner_task, jnp.where(along_io, N_COMP + owner_group, 127))
    rows = lax.broadcasted_iota(jnp.int32, (KEYS, 128), 0)
    for b in range(BLOCKS):
        hit = rows == key[b : b + 1, :]
        onehot[b * KEYS : (b + 1) * KEYS, :] = jnp.where(hit, 1.0, 0.0).astype(jnp.bfloat16)
    r = lax.broadcasted_iota(jnp.int32, (128, 256), 0)
    c = lax.broadcasted_iota(jnp.int32, (128, 256), 1)
    earlier = jnp.where((r < c) | (c >= 128), 1.0, 0.0).astype(jnp.bfloat16)
    prefix[...] = jnp.dot(onehot[...], earlier, preferred_element_type=jnp.float32)
    carry = jnp.zeros((KEYS, 128), jnp.float32)
    for b in range(BLOCKS):
        hit = rows == key[b : b + 1, :]
        counted = prefix[b * KEYS : (b + 1) * KEYS, 0:128] + carry
        ranks[b : b + 1, :] = jnp.sum(jnp.where(hit, counted, 0.0), axis=0, keepdims=True)
        carry = carry + prefix[b * KEYS : (b + 1) * KEYS, 128:256]
    rank = ranks[...].astype(jnp.int32)
    upper = (task + 1) & (N_COMP - 1)
    after = (group + 1) & (N_IO - 1)
    before = (group + N_IO - 1) & (N_IO - 1)
    comp_slot = jnp.where(
        rank < SPREAD,
        owner_task * SPREAD + rank,
        jnp.where(owner_task == upper, 512, 768) + rank - SPREAD,
    )
    io_slot = (
        jnp.where(owner_group == after, 1024, jnp.where(owner_group == before, 1280, 1536)) + rank
    )
    slot = jnp.where(along_comp, comp_slot, jnp.where(along_io, io_slot, 2047))
    stay_ref[...] = 2 * jnp.where(along_comp | along_io, DUMP, position)
    write_stay = pltpu.make_async_copy(stay_ref, stay_out, sems.at[7])
    slot_high = slot >> 7
    slot_low = slot & 127
    column = lax.broadcasted_iota(jnp.int32, (BLOCKS, 128), 0) * 128 + lax.broadcasted_iota(
        jnp.int32, (BLOCKS, 128), 1
    )
    coded = position + 1
    parts = [
        (column & 255).astype(jnp.float32),
        (column >> 8).astype(jnp.float32),
        (coded & 255).astype(jnp.float32),
        (coded >> 8).astype(jnp.float32),
    ]
    rows16 = lax.broadcasted_iota(jnp.int32, (16, 128), 0)
    rows128 = lax.broadcasted_iota(jnp.int32, (128, 128), 0)
    for b in range(BLOCKS):
        hit = rows16 == slot_high[b : b + 1, :]
        for j in range(4):
            high[16 * j : 16 * (j + 1), 128 * b : 128 * (b + 1)] = jnp.where(
                hit, parts[j][b : b + 1, :], 0.0
            ).astype(jnp.bfloat16)
        low[:, 128 * b : 128 * (b + 1)] = jnp.where(
            rows128 == slot_low[b : b + 1, :], 1.0, 0.0
        ).astype(jnp.bfloat16)
    found = lax.dot_general(
        high[...], low[...], (((1,), (1,)), ((), ())), preferred_element_type=jnp.float32
    )
    chosen = (found[0:16, :] + 256.0 * found[16:32, :]).astype(jnp.int32)
    source[...] = (chosen >> 3) * 16 + (chosen & 7)
    push = pltpu.make_async_copy(source, source_s, sems.at[1])
    push.start()
    write_stay.start()
    coded = found[32:48, :] + 256.0 * found[48:64, :]
    goal = jnp.where(coded > 0.5, coded - 1.0, float(DUMP)).astype(jnp.int32)
    goal = ((goal >> 3) * 16 + (goal & 7)).astype(jnp.float32)
    turned = pltpu.roll(goal, (task & 15) * SPREAD, 1)
    for j in range(16):
        row = pltpu.roll(turned, (128 - SPREAD * j) % 128, 1)
        for g in range(N_COMP // 16):
            at = PACKET * (16 * g + j) + 2 * SPREAD
            spread_ref[at : at + 1, :] = row[g : g + 1, :]
    up_ref[0:2, :] = goal[4:6, :]
    down_ref[0:2, :] = goal[6:8, :]
    next_ref[0:2, :] = goal[8:10, :]
    prev_ref[0:2, :] = goal[10:12, :]
    far_ref[0:1, :] = goal[12:13, :]
    push.wait()
    fetch.wait()

    def copy(into, at, slot):
        row = source_s[slot // 128, slot % 128]
        into[pl.ds(at, 2), :] = fields[pl.ds(row, 2, stride=8), :]

    part = N_COMP * PACKET // 4
    writes = []
    for q in range(4):
        for s in range(128 * q, 128 * (q + 1)):
            copy(spread_ref, PACKET * (s // SPREAD) + 2 * (s % SPREAD), s)
        write = pltpu.make_async_copy(
            spread_ref.at[pl.ds(part * q, part), :],
            spread_out.at[pl.ds(part * q, part), :],
            sems.at[3 + q],
        )
        write.start()
        writes.append(write)
    for s in range(NEAR_COMP):
        copy(up_ref, 2 + 2 * s, 512 + s)
    for s in range(NEAR_COMP):
        copy(down_ref, 2 + 2 * s, 768 + s)
    for s in range(NEAR_IO):
        copy(next_ref, 2 + 2 * s, 1024 + s)
    for s in range(NEAR_IO):
        copy(prev_ref, 2 + 2 * s, 1280 + s)
    for s in range(SPREAD):
        copy(far_ref, 1 + 2 * s, 1536 + s)
    write_stay.wait()
    for write in writes:
        write.wait()


def remap(x, high_ref, low_ref):
    x_high = x.astype(jnp.bfloat16)
    x_low = (x - x_high.astype(jnp.float32)).astype(jnp.bfloat16)
    total = jnp.dot(x_high, high_ref[...], preferred_element_type=jnp.float32)
    total += jnp.dot(x_high, low_ref[...], preferred_element_type=jnp.float32)
    total += jnp.dot(x_low, high_ref[...], preferred_element_type=jnp.float32)
    return total


def local_kernel(
    stay_in, fields_in, remap_ref, kept_ref, high_ref, low_ref, fields, placed, result, stay, sems
):
    fetch_stay = pltpu.make_async_copy(stay_in, stay, sems.at[4])
    fetch_stay.start()
    part = 2 * COLUMNS // 4
    fetches = []
    for q in range(4):
        fetch = pltpu.make_async_copy(
            fields_in.at[pl.ds(part * q, part), :],
            fields.at[pl.ds(part * q, part), :],
            sems.at[q],
        )
        fetch.start()
        fetches.append(fetch)
    zero = jnp.zeros((64, 64), jnp.float32)
    for f in range(4):
        band = jnp.concatenate([remap_ref[f] if g == f else zero for g in range(4)], axis=1)
        top = band.astype(jnp.bfloat16)
        high_ref[64 * f : 64 * (f + 1), :] = top
        low_ref[64 * f : 64 * (f + 1), :] = (band - top.astype(jnp.float32)).astype(jnp.bfloat16)
    fetch_stay.wait()
    for q, fetch in enumerate(fetches):
        fetch.wait()
        for c in range(COLUMNS // 4 * q, COLUMNS // 4 * (q + 1)):
            row = 16 * (c // 8) + c % 8
            placed[pl.ds(stay[c // 128, c % 128], 2), :] = fields[pl.ds(row, 2, stride=8), :]
    writes = []
    size = 512
    for j in range(COLUMNS // size):
        left = placed[pl.ds(2 * size * j, size, stride=2), :]
        right = placed[pl.ds(2 * size * j + 1, size, stride=2), :]
        result[size * j : size * (j + 1), :] = remap(
            jnp.concatenate([left, right], axis=1), high_ref, low_ref
        )
        write = pltpu.make_async_copy(
            result.at[pl.ds(size * j, size), :],
            kept_ref.at[pl.ds(size * j, size), :],
            sems.at[5 + j],
        )
        write.start()
        writes.append(write)
    for write in writes:
        write.wait()


def final_kernel(
    spread_ref,
    up_ref,
    down_ref,
    next_ref,
    prev_ref,
    far_ref,
    kept_in,
    high_ref,
    low_ref,
    out_ref,
    kept,
    goal,
    goal_s,
    mixed,
    sems,
):
    part = 2 * COLUMNS // 4
    fetches = []
    for q in range(4):
        fetch = pltpu.make_async_copy(
            kept_in.at[pl.ds(part * q, part), :], kept.at[pl.ds(part * q, part), :], sems.at[1 + q]
        )
        fetch.start()
        fetches.append(fetch)
    rows = jnp.concatenate(
        [spread_ref[PACKET * t + 2 * SPREAD : PACKET * (t + 1), :] for t in range(N_COMP)], axis=0
    )
    packet = lax.broadcasted_iota(jnp.int32, (N_COMP, 128), 0)
    lane = lax.broadcasted_iota(jnp.int32, (N_COMP, 128), 1)
    rows = jnp.where((packet & 15) == (lane >> 3), rows, 0.0)
    goal[0:4, :] = jnp.sum(rows.reshape(4, 16, 128), axis=1).astype(jnp.int32)
    for j, ref in enumerate((up_ref, down_ref, next_ref, prev_ref)):
        goal[4 + 2 * j : 6 + 2 * j, :] = ref[0:2, :].astype(jnp.int32)
    goal[12:13, :] = far_ref[0:1, :].astype(jnp.int32)
    push = pltpu.make_async_copy(goal, goal_s, sems.at[0])
    push.start()

    def halves(ref, first, count, stride, step):
        return jnp.concatenate(
            [ref[pl.ds(first, count, stride=stride), :], ref[pl.ds(first + step, count, stride=stride), :]],
            axis=1,
        )

    @pl.when(lax.axis_index("comp") >= 0)
    def _():
        groups = [
            [halves(spread_ref, 2 * k, N_COMP, PACKET, 1) for k in range(SPREAD)],
            [halves(ref, 2, NEAR_COMP, 2, 1) for ref in (up_ref, down_ref)],
            [halves(ref, 2, NEAR_IO, 2, 1) for ref in (next_ref, prev_ref)]
            + [halves(far_ref, 1, SPREAD, 2, 1)],
        ]
        at = 0
        for group in groups:
            total = remap(jnp.concatenate(group, axis=0), high_ref, low_ref)
            for g in range(total.shape[0] // 8):
                mixed[at : at + 8, :] = total[8 * g : 8 * (g + 1), 0:128]
                mixed[at + 8 : at + 16, :] = total[8 * g : 8 * (g + 1), 128:256]
                at += 16

    push.wait()
    for fetch in fetches:
        fetch.wait()

    def copy(row, slot):
        kept[pl.ds(goal_s[slot // 128, slot % 128], 2, stride=8), :] = mixed[
            pl.ds(16 * (row // 8) + row % 8, 2, stride=8), :
        ]

    for s in range(N_COMP * SPREAD):
        copy(N_COMP * (s % SPREAD) + s // SPREAD, s)
    row = N_COMP * SPREAD
    for base, count in ((512, NEAR_COMP), (768, NEAR_COMP), (1024, NEAR_IO), (1280, NEAR_IO), (1536, SPREAD)):
        for s in range(count):
            copy(row + s, base + s)
        row += count
    writes = []
    for q in range(4):
        write = pltpu.make_async_copy(
            kept.at[pl.ds(part * q, part), :], out_ref.at[pl.ds(part * q, part), :], sems.at[1 + q]
        )
        write.start()
        writes.append(write)
    for write in writes:
        write.wait()


def shift(value, axis, by):
    peers = lax.axis_size(axis)
    return lax.ppermute(value, axis, [(i, (i + by) % peers) for i in range(peers)])


def per_device(fields, file_offset, level_remap):
    f32 = jnp.float32
    whole = pl.BlockSpec(memory_space=VMEM)
    anywhere = pl.BlockSpec(memory_space=pl.ANY)
    fields = (
        fields.reshape(COLUMNS // 8, 8, 2, 128).transpose(0, 2, 1, 3).reshape(2 * COLUMNS, 128)
    )
    fields = pltpu.with_memory_space_constraint(fields, pltpu.HBM)
    file_offset = pltpu.with_memory_space_constraint(file_offset, pltpu.HBM)
    spread, up, down, after, before, far, stay = pl.pallas_call(
        pack_kernel,
        name="pack",
        out_shape=[
            pltpu.HBM((N_COMP * PACKET, 128), f32),
            VMEM((COMP_ROWS, 128), f32),
            VMEM((COMP_ROWS, 128), f32),
            VMEM((IO_ROWS, 128), f32),
            VMEM((IO_ROWS, 128), f32),
            VMEM((FAR_ROWS, 128), f32),
            pltpu.HBM((BLOCKS, 128), jnp.int32),
        ],
        in_specs=[anywhere, anywhere],
        out_specs=[anywhere] + [whole] * 5 + [anywhere],
        scratch_shapes=[
            VMEM((2 * COLUMNS, 128), f32),
            VMEM((BLOCKS, 128), jnp.int32),
            VMEM((BLOCKS, 128), jnp.int32),
            VMEM((N_COMP * PACKET, 128), f32),
            VMEM((BLOCKS * KEYS, 128), jnp.bfloat16),
            VMEM((BLOCKS * KEYS, 256), f32),
            VMEM((BLOCKS, 128), f32),
            VMEM((64, COLUMNS), jnp.bfloat16),
            VMEM((128, COLUMNS), jnp.bfloat16),
            VMEM((16, 128), jnp.int32),
            SMEM((16, 128), jnp.int32),
            pltpu.SemaphoreType.DMA((8,)),
        ],
        compiler_params=pltpu.CompilerParams(vmem_limit_bytes=40 * 2**20),
        cost_estimate=pl.CostEstimate(flops=20_000_000, bytes_accessed=5_000_000, transcendentals=0),
    )(file_offset, fields)
    spread = lax.all_to_all(
        spread.reshape(N_COMP, 1, PACKET * 128), "comp", split_axis=0, concat_axis=0, tiled=True
    ).reshape(N_COMP * PACKET, 128)
    up = shift(up, "comp", 1)
    down = shift(down, "comp", -1)
    after = shift(after, "io", 1)
    before = shift(before, "io", -1)
    far = shift(far, "io", 2)
    kept, high, low = pl.pallas_call(
        local_kernel,
        name="local",
        out_shape=[
            pltpu.HBM((COLUMNS, WIDTH), f32),
            VMEM((WIDTH, WIDTH), jnp.bfloat16),
            VMEM((WIDTH, WIDTH), jnp.bfloat16),
        ],
        in_specs=[anywhere, anywhere, whole],
        out_specs=[anywhere, whole, whole],
        scratch_shapes=[
            VMEM((2 * COLUMNS, 128), f32),
            VMEM((PLACED, 128), f32),
            VMEM((COLUMNS, WIDTH), f32),
            SMEM((BLOCKS, 128), jnp.int32),
            pltpu.SemaphoreType.DMA((5 + COLUMNS // 512,)),
        ],
        compiler_params=pltpu.CompilerParams(vmem_limit_bytes=40 * 2**20),
        cost_estimate=pl.CostEstimate(flops=4_000_000_000, bytes_accessed=6_000_000, transcendentals=0),
    )(pltpu.with_memory_space_constraint(stay, pltpu.HBM), fields, level_remap)
    kept = kept.reshape(COLUMNS // 8, 8, 2, 128).transpose(0, 2, 1, 3).reshape(2 * COLUMNS, 128)
    operands = [
        pltpu.with_memory_space_constraint(x, VMEM)
        for x in (spread, up, down, after, before, far, high, low)
    ]
    operands.insert(6, pltpu.with_memory_space_constraint(kept, pltpu.HBM))
    out = pl.pallas_call(
        final_kernel,
        name="final",
        out_shape=jax.ShapeDtypeStruct((2 * COLUMNS, 128), f32),
        in_specs=[whole] * 6 + [anywhere, whole, whole],
        out_specs=anywhere,
        scratch_shapes=[
            VMEM((PLACED, 128), f32),
            VMEM((16, 128), jnp.int32),
            SMEM((16, 128), jnp.int32),
            VMEM((2 * RECEIVED, 128), f32),
            pltpu.SemaphoreType.DMA((5,)),
        ],
        compiler_params=pltpu.CompilerParams(vmem_limit_bytes=40 * 2**20),
        cost_estimate=pl.CostEstimate(flops=1_000_000_000, bytes_accessed=8_000_000, transcendentals=0),
    )(*operands)
    return out.reshape(COLUMNS // 8, 2, 8, 128).transpose(0, 2, 1, 3).reshape(COLUMNS, WIDTH)


def solution(mesh):
    placed = (P(("io", "comp"), None), P(("io", "comp"), None), P())

    return jax.shard_map(
        per_device, mesh=mesh, in_specs=placed, out_specs=P(("io", "comp"), None), check_vma=False
    )
```
